32 devices in a mesh: grp: 2 (over y), dev: 16 (over z, x, core).
Axes of the slice: x: 2, y: 2, z: 4, core: 2. Of those that a mesh axis runs over, the one named last changes fastest.
Arguments:
- pooled_grad: bfloat16 [4096, 32, 128], P(('grp', 'dev')), may hold values from -6 to 6
- row_ids: int32 [4096, 4, 32], P(('grp', 'dev')), may hold values from 0 to 1023
- scale_exps: int32 [4096, 32], P(('grp', 'dev')), may hold values from 0 to 3
- table_owner: int32 [32], replicated, may hold values from 0 to 31, each once
- dense_acts: bfloat16 [4096, 512], P(('grp', 'dev')), may hold values from -6 to 6
- dense_cot: bfloat16 [4096, 512], P(('grp', 'dev')), may hold values from -0.1875 to 0.1875
Outputs:
- table_grad: float32 [32, 1024, 128], P('dev')
- weight_grad: float32 [512, 512], replicated
- bias_grad: float32 [512], replicated
The draws below stay inside these ranges and needn't reach their ends.
Inputs may be any that keep to these rules, and one draw needn't show every extreme that they name: Table t's rows are accumulated into slot table_owner[t]; each slot belongs to exactly one table.
All inputs are finite; a program needn't handle non-finite values.
Results may differ from the reference program's by a relative error of at most 0.0003.
Values may be sent and summed in bfloat16 or wider, within the bound.
A program may use at most 128 MiB of HBM per device.

```python
import jax
import jax.numpy as jnp
from jax import lax

E = 128
POOL = 4
HID = 512
HID2 = 512
ROWS = 1024
TABLES = 32
BATCH = 4096


def plant(array, own_key, smallest, top_value):
    longest = array.shape.index(max(array.shape))
    spots = []
    for shift in (0, 1):
        where = [jax.random.randint(jax.random.fold_in(own_key, axis), (), 0, length) for axis, length in enumerate(array.shape)]
        where[longest] = (where[longest] + shift) % array.shape[longest]
        spots.append(tuple(where))
    return array.at[spots[0]].set(smallest).at[spots[1]].set(top_value)


def raised(entries, stream_key, source, target, blocks, factor):
    def block_of(axis_at):
        return (jnp.arange(entries.shape[axis_at]) // (entries.shape[axis_at] // blocks)).reshape((-1,) + (1,) * (entries.ndim - 1 - axis_at))

    one_side = jax.random.permutation(stream_key, blocks)[block_of(target)]
    far = (block_of(target) + blocks // 2) % blocks
    return jnp.where((block_of(source) == one_side) | (block_of(source) == far), factor * entries, entries)


def shard_levels(key, dims, split, low, high):
    def one(position, blocks):
        steps = jax.random.uniform(jax.random.fold_in(jax.random.fold_in(key, 6), position), (blocks,), jnp.float32, low / len(split), high / len(split))
        return jnp.repeat(jnp.exp(steps), dims[position] // blocks).reshape((-1,) + (1,) * (len(dims) - position - 1))

    gain = one(*split[0])
    for cut in split[1:]:
        gain = gain * one(*cut)
    return gain


def normal_values(rng, extent, spread, most, pieces=(), kind=jnp.bfloat16):
    array = jax.random.normal(rng, extent, jnp.float32) * spread
    if len(pieces) > 0:
        array = shard_levels(rng, extent, pieces, -0.22, 0.18) * array
    return jnp.clip(array, min=-most, max=most).astype(kind)


def heavy_noise(key, extent, spread, bound, pieces, heavy, kind=jnp.bfloat16):
    array = spread * jax.random.normal(key, extent, jnp.float32)
    if pieces:
        array = array * shard_levels(key, extent, pieces, -0.22, 0.18)
    return jnp.clip(raised(array, jax.random.fold_in(key, 3), *heavy), -bound, bound).astype(kind)


def setup_inputs(seed: int = 0) -> dict:
    arg_keys = jax.random.split(jax.random.key(seed), 7)
    pooled_grad = normal_values(arg_keys[0], (BATCH, TABLES, E), 1.0, 6.0, ((0, 32),))
    row_ids = plant(jax.random.randint(arg_keys[1], (BATCH, POOL, TABLES), 0, ROWS), jax.random.fold_in(arg_keys[1], 1), 0, ROWS - 1).astype(jnp.int32)
    scale_exps = plant(jax.random.randint(arg_keys[2], (BATCH, TABLES), 0, 4), jax.random.fold_in(arg_keys[2], 1), 0, 3).astype(jnp.int32)
    table_owner = jax.random.permutation(arg_keys[3], TABLES).astype(jnp.int32)
    dense_acts = normal_values(arg_keys[4], (BATCH, HID), 1.0, 6.0, ((0, 32),))
    dense_cot = heavy_noise(arg_keys[5], (BATCH, HID2), BATCH ** -0.5, 0.1875, ((0, 32),), (0, 1, 32, 2.75))
    return dict(pooled_grad=pooled_grad, row_ids=row_ids, scale_exps=scale_exps, table_owner=table_owner, dense_acts=dense_acts, dense_cot=dense_cot)


def powers(exps):
    return (1.0 + (exps >= 1).astype(jnp.float32) + 2.0 * (exps >= 2).astype(jnp.float32)
            + 4.0 * (exps >= 3).astype(jnp.float32))


def reference(pooled_grad, row_ids, scale_exps, table_owner, dense_acts, dense_cot):
    factor = powers(scale_exps)
    quantized = jnp.clip(pooled_grad.astype(jnp.float32) / factor[:, :, None], -1.0, 1.0).astype(jnp.bfloat16)
    restored = (quantized.astype(jnp.float32) * factor[:, :, None]).astype(jnp.bfloat16)

    def per_table(column):
        values = jnp.take(restored, column, axis=1).astype(jnp.float32)
        indices = jnp.take(row_ids, column, axis=2).astype(jnp.int32)
        summed = jnp.zeros((ROWS, E), jnp.float32)
        for lookup in range(POOL):
            summed = summed.at[indices[:, lookup]].add(values)
        return summed

    by_table = lax.map(per_table, jnp.arange(TABLES, dtype=jnp.int32))
    table_grad = jnp.zeros_like(by_table).at[table_owner].set(by_table)
    weight_grad = lax.dot_general(dense_acts, dense_cot, (((0,), (0,)), ((), ())),
                                  preferred_element_type=jnp.float32)
    bias_grad = jnp.sum(dense_cot.astype(jnp.float32), axis=0)
    return table_grad, weight_grad, bias_grad
```

```python
import functools

import jax
import jax.numpy as jnp
from jax import lax
from jax.experimental import pallas as pl
from jax.experimental.pallas import tpu as pltpu
from jax.sharding import PartitionSpec as P

ROWS = 1024
DIGIT = 32
MESH = pl.DeviceIdType.MESH
ROW_BLOCK = 256


def powers(exps):
    return (
        1.0
        + (exps >= 1).astype(jnp.float32)
        + 2.0 * (exps >= 2).astype(jnp.float32)
        + 4.0 * (exps >= 3).astype(jnp.float32)
    )


def kernel(
    devs,
    pool,
    slot_ref,
    x_ref,
    ids_ref,
    acts_ref,
    cot_ref,
    table_ref,
    weight_ref,
    bias_ref,
    send,
    recv,
    part,
    whole,
    half0,
    half1,
    half2,
    zbuf,
    bpart,
    bhalf,
    bz,
    asend,
    arecv,
    fsend,
    frecv,
    dsend,
    drecv,
    esend,
    erecv,
    zsend,
    zrecv,
    bsend,
    brecv,
    gsend,
    grecv,
):
    me = lax.axis_index("dev")
    grp = lax.axis_index("grp")
    other = 1 - grp
    owned, samples, feat = table_ref.shape[0], x_ref.shape[1], x_ref.shape[2]
    id_rows = ids_ref.shape[1]
    zs = devs // 4
    core = lax.rem(me, 2)
    xbit = lax.rem(lax.div(me, 2), 2)
    z = lax.div(me, 4)
    hid, hid2 = weight_ref.shape
    wide = hid2 // 128
    total = hid * wide

    def remote(src, dst, ssem, rsem, dev, group):
        return pltpu.make_async_remote_copy(
            src_ref=src,
            dst_ref=dst,
            send_sem=ssem,
            recv_sem=rsem,
            device_id={"grp": group, "dev": dev},
            device_id_type=MESH,
        )

    for j in range(wide):
        part[pl.ds(j * hid, hid), :] = lax.dot_general(
            acts_ref[...],
            cot_ref[:, j * 128 : (j + 1) * 128],
            (((0,), (0,)), ((), ())),
            preferred_element_type=jnp.float32,
        )
    bpart[0] = jnp.zeros(bpart.shape[1:], jnp.float32)
    for j in range(wide):
        bpart[0, j : j + 1, :] = jnp.sum(
            cot_ref[:, j * 128 : (j + 1) * 128].astype(jnp.float32), axis=0, keepdims=True
        )

    near = me + 1 - 2 * core
    across = me + 2 - 4 * xbit
    stages = (
        (near, grp, core, half0),
        (across, grp, xbit, half1),
        (me, other, grp, half2),
    )
    bases = [0]
    for s in range(3):
        size = total >> (s + 1)
        bases.append(bases[s] + stages[s][2] * size)

    def halving(s):
        dev, group, bit, landing = stages[s]
        size = total >> (s + 1)
        away = pl.multiple_of(bases[s] + (1 - bit) * size, 8)
        return (
            remote(
                part.at[pl.ds(away, size)], landing, dsend.at[s], drecv.at[s], dev, group
            ),
            remote(bpart.at[s], bhalf.at[s], bsend.at[s], brecv.at[s], dev, group),
        )

    def halving_start(s):
        for copy in halving(s):
            copy.start()

    def halving_finish(s):
        for copy in halving(s):
            copy.wait()
        size = total >> (s + 1)
        keep = pl.multiple_of(bases[s + 1], 8)
        part[pl.ds(keep, size), :] = part[pl.ds(keep, size), :] + stages[s][3][...]
        bpart[s + 1] = bpart[s] + bhalf[s]

    piece = (total >> 3) // zs

    def z_copy(k):
        peer = lax.rem(z + k, zs)
        dev = peer * 4 + lax.rem(me, 4)
        away = pl.multiple_of(bases[3] + peer * piece, 8)
        return (
            remote(
                part.at[pl.ds(away, piece)], zbuf.at[z], zsend.at[peer], zrecv.at[z], dev, grp
            ),
            remote(bpart.at[3], bz.at[z], bsend.at[3 + peer], brecv.at[3 + z], dev, grp),
        )

    def z_wait(k):
        peer = lax.rem(z + k, zs)
        dev = peer * 4 + lax.rem(me, 4)
        here = pl.multiple_of(bases[3] + z * piece, 8)
        return (
            remote(
                part.at[pl.ds(here, piece)], zbuf.at[peer], zsend.at[peer], zrecv.at[peer], dev, grp
            ),
            remote(bpart.at[3], bz.at[peer], bsend.at[3 + peer], brecv.at[3 + peer], dev, grp),
        )

    mine = pl.multiple_of(bases[3] + z * piece, 8)

    def z_start():
        @pl.loop(1, zs)
        def _(k):
            for copy in z_copy(k):
                copy.start()

    def z_finish():
        zbuf[z] = part[pl.ds(mine, piece), :]
        bz[z] = bpart[3]

        @pl.loop(1, zs)
        def _(k):
            for copy in z_wait(k):
                copy.wait_recv()

        @pl.loop(1, zs)
        def _(k):
            for copy in z_copy(k):
                copy.wait_send()

        whole[pl.ds(mine, piece), :] = lax.fori_loop(
            1, zs, lambda i, run: run + zbuf[i], zbuf[0]
        )
        bsum = lax.fori_loop(1, zs, lambda i, run: run + bz[i], bz[0])
        for j in range(wide):
            bias_ref[:, j * 128 : (j + 1) * 128] = bsum[j : j + 1, :]

    def zg_copy(k, back):
        peer = lax.rem(z + k, zs)
        dev = peer * 4 + lax.rem(me, 4)
        off = mine if not back else pl.multiple_of(bases[3] + peer * piece, 8)
        block = whole.at[pl.ds(off, piece)]
        return remote(block, block, gsend.at[peer], grecv.at[peer if back else z], dev, grp)

    def zg_start():
        @pl.loop(1, zs)
        def _(k):
            zg_copy(k, False).start()

    def zg_finish():
        @pl.loop(1, zs)
        def _(k):
            zg_copy(k, True).wait_recv()

        @pl.loop(1, zs)
        def _(k):
            zg_copy(k, False).wait_send()

    def doubling(s, back):
        dev, group, bit, _ = stages[s]
        size = total >> (s + 1)
        off = bases[s] + (1 - bit) * size if back else bases[s + 1]
        block = whole.at[pl.ds(pl.multiple_of(off, 8), size)]
        return remote(block, block, esend.at[s], erecv.at[s], dev, group)

    def doubling_start(s):
        doubling(s, False).start()

    def doubling_finish(s):
        doubling(s, True).wait_recv()
        doubling(s, False).wait_send()

    halving_start(0)

    def chunk_copy(k):
        dst = lax.rem(me + k, devs)
        return remote(
            send.at[dst], recv.at[0, me], asend.at[dst], arecv.at[me], dst, grp
        )

    def arrival(k):
        src = lax.rem(me - k + devs, devs)
        return remote(
            send.at[src], recv.at[0, src], asend.at[src], arecv.at[src], src, grp
        )

    def forward(k):
        src = lax.rem(me - k + devs, devs)
        return remote(
            recv.at[0, src], recv.at[1, src], fsend.at[src], frecv.at[src], me, other
        )

    def build(k):
        dst = lax.rem(me + k, devs)
        digits = []
        for s in range(owned):
            t = slot_ref[dst * owned + s]
            send[dst, pl.ds(s * samples, samples), :] = x_ref[t]
            digits.append(ids_ref[t])
        send[dst, pl.ds(owned * samples, owned * id_rows), :] = jnp.concatenate(
            digits, axis=0
        ).astype(jnp.bfloat16)

    build(0)
    recv[0, me] = send[me]

    @pl.loop(1, devs)
    def _(k):
        build(k)
        chunk_copy(k).start()

    forward(0).start()
    table_ref[...] = jnp.zeros(table_ref.shape, jnp.float32)

    def accumulate(side, j):
        first = lax.rem(me - 2 * j + devs, devs)
        second = lax.rem(me - 2 * j - 1 + devs, devs)
        digits = jnp.concatenate(
            [
                recv[side, c, pl.ds(owned * samples, owned * id_rows), :].astype(jnp.float32)
                for c in (first, second)
            ],
            axis=1,
        )
        for s in range(owned):
            top = digits[s * id_rows : s * id_rows + pool]
            low = digits[s * id_rows + pool : s * id_rows + 2 * pool]
            rows = top * DIGIT + low
            values = jnp.concatenate(
                [recv[side, c, pl.ds(s * samples, samples), :] for c in (first, second)],
                axis=0,
            )
            for block in range(ROWS // ROW_BLOCK):
                local = rows - block * ROW_BLOCK
                local = jnp.where((local >= 0) & (local < ROW_BLOCK), local, -1.0).astype(
                    jnp.bfloat16
                )
                axis = lax.broadcasted_iota(
                    jnp.int32, (ROW_BLOCK, 2 * samples), 0
                ).astype(jnp.float32).astype(jnp.bfloat16)
                one, zero = jnp.bfloat16(1), jnp.bfloat16(0)
                counts = jnp.where(local[0:1] == axis, one, zero)
                for p in range(1, pool):
                    counts = counts + jnp.where(local[p : p + 1] == axis, one, zero)
                span = pl.ds(block * ROW_BLOCK, ROW_BLOCK)
                table_ref[s, span, :] = table_ref[s, span, :] + jnp.dot(
                    counts, values, preferred_element_type=jnp.float32
                )

    pairs = devs // 2
    cuts = [0, pairs // 4, pairs // 2, 3 * pairs // 4, pairs]

    def own_loop(seg):
        @pl.loop(cuts[seg], cuts[seg + 1])
        def _(j):
            for k in (2 * j, 2 * j + 1):

                @pl.when(k > 0)
                def _(k=k):
                    arrival(k).wait_recv()
                    forward(k).start()

            accumulate(0, j)

    def far_loop(seg):
        @pl.loop(cuts[seg], cuts[seg + 1])
        def _(j):
            for k in (2 * j, 2 * j + 1):
                src = lax.rem(me - k + devs, devs)
                remote(
                    recv.at[0, src], recv.at[1, src], fsend.at[src], frecv.at[src], me, other
                ).wait_recv()
            accumulate(1, j)

    halving_finish(0)
    halving_start(1)
    own_loop(0)
    halving_finish(1)
    halving_start(2)
    own_loop(1)
    halving_finish(2)
    z_start()
    own_loop(2)
    z_finish()
    zg_start()
    own_loop(3)
    zg_finish()
    doubling_start(2)
    far_loop(0)
    doubling_finish(2)
    doubling_start(1)
    far_loop(1)
    far_loop(2)
    doubling_finish(1)
    doubling_start(0)
    far_loop(3)
    doubling_finish(0)
    for j in range(wide):
        weight_ref[:, j * 128 : (j + 1) * 128] = whole[pl.ds(j * hid, hid), :]

    @pl.loop(1, devs)
    def _(k):
        chunk_copy(k).wait_send()

    @pl.loop(0, devs)
    def _(k):
        forward(k).wait_send()


def solution(mesh):
    devs = mesh.shape["dev"]

    def per_device(pooled_grad, row_ids, scale_exps, table_owner, dense_acts, dense_cot):
        samples, tables, feat = pooled_grad.shape
        pool = row_ids.shape[1]
        owned = tables // devs
        hid, hid2 = dense_acts.shape[1], dense_cot.shape[1]
        zs = devs // 4
        factor = powers(scale_exps)[:, :, None]
        restored = jnp.transpose(
            jnp.clip(pooled_grad.astype(jnp.float32), -factor, factor).astype(jnp.bfloat16),
            (1, 0, 2),
        )
        by_table = jnp.transpose(row_ids, (2, 1, 0))
        digits = jnp.concatenate([by_table // DIGIT, by_table % DIGIT], axis=1).astype(jnp.float32)
        order = jnp.arange(tables, dtype=jnp.int32)
        slots = jnp.sum(
            jnp.where(table_owner[None, :] == order[:, None], order[None, :], 0), axis=1
        ).astype(jnp.int32)
        rows = owned * samples + owned * digits.shape[1]
        total = hid * hid2 // 128
        dma = pltpu.SemaphoreType.DMA
        vmem = pl.BlockSpec(memory_space=pltpu.VMEM)
        table_grad, weight_grad, bias_grad = pl.pallas_call(
            functools.partial(kernel, devs, pool),
            out_shape=(
                jax.ShapeDtypeStruct((owned, ROWS, feat), jnp.float32),
                jax.ShapeDtypeStruct((hid, hid2), jnp.float32),
                jax.ShapeDtypeStruct((1, hid2), jnp.float32),
            ),
            in_specs=[pl.BlockSpec(memory_space=pltpu.SMEM)] + [vmem] * 4,
            out_specs=(vmem, vmem, vmem),
            scratch_shapes=[
                pltpu.VMEM((devs, rows, feat), jnp.bfloat16),
                pltpu.VMEM((2, devs, rows, feat), jnp.bfloat16),
                pltpu.VMEM((total, 128), jnp.float32),
                pltpu.VMEM((total, 128), jnp.float32),
                pltpu.VMEM((total // 2, 128), jnp.float32),
                pltpu.VMEM((total // 4, 128), jnp.float32),
                pltpu.VMEM((total // 8, 128), jnp.float32),
                pltpu.VMEM((zs, total // 8 // zs, 128), jnp.float32),
                pltpu.VMEM((4, 8, 128), jnp.float32),
                pltpu.VMEM((3, 8, 128), jnp.float32),
                pltpu.VMEM((zs, 8, 128), jnp.float32),
                dma((devs,)),
                dma((devs,)),
                dma((devs,)),
                dma((devs,)),
                dma((3,)),
                dma((3,)),
                dma((3,)),
                dma((3,)),
                dma((zs,)),
                dma((zs,)),
                dma((3 + zs,)),
                dma((3 + zs,)),
                dma((zs,)),
                dma((zs,)),
            ],
            compiler_params=pltpu.CompilerParams(has_side_effects=True),
        )(slots, restored, digits, dense_acts, dense_cot)
        return table_grad, weight_grad, bias_grad.reshape(hid2)

    return jax.shard_map(
        per_device,
        mesh=mesh,
        in_specs=(
            P(("grp", "dev"), None, None),
            P(("grp", "dev"), None, None),
            P(("grp", "dev"), None),
            P(),
            P(("grp", "dev"), None),
            P(("grp", "dev"), None),
        ),
        out_specs=(P("dev", None, None), P(), P()),
        check_vma=False,
    )
```

```python
import functools

import jax
import jax.numpy as jnp
from jax import lax
from jax.experimental import pallas as pl
from jax.experimental.pallas import tpu as pltpu
from jax.sharding import PartitionSpec as P

ROWS = 1024
DIGIT_BITS = 5
DIGIT = 1 << DIGIT_BITS
MESH = pl.DeviceIdType.MESH
ROW_BLOCK = 256


def powers(exps):
    return (
        1.0
        + (exps >= 1).astype(jnp.float32)
        + 2.0 * (exps >= 2).astype(jnp.float32)
        + 4.0 * (exps >= 3).astype(jnp.float32)
    )


def kernel(
    devs,
    pool,
    slot_ref,
    x_ref,
    ids_ref,
    acts_ref,
    cot_ref,
    table_ref,
    weight_ref,
    bias_ref,
    send,
    recv,
    inter,
    part,
    whole,
    half0,
    half1,
    half2,
    zbuf,
    bpart,
    bhalf,
    bz,
    psend,
    precv,
    csend,
    crecv,
    fsend,
    frecv,
    dsend,
    drecv,
    esend,
    erecv,
    zsend,
    zrecv,
    bsend,
    brecv,
    gsend,
    grecv,
):
    me = lax.axis_index("dev")
    grp = lax.axis_index("grp")
    other = 1 - grp
    owned, samples, feat = table_ref.shape[0], x_ref.shape[1], x_ref.shape[2]
    id_rows = 2 * ids_ref.shape[1]
    zs = devs // 4
    core = lax.rem(me, 2)
    xbit = lax.rem(lax.div(me, 2), 2)
    z = lax.div(me, 4)
    hid, hid2 = weight_ref.shape
    wide = hid2 // 128
    total = hid * wide

    def remote(src, dst, ssem, rsem, dev, group):
        return pltpu.make_async_remote_copy(
            src_ref=src,
            dst_ref=dst,
            send_sem=ssem,
            recv_sem=rsem,
            device_id={"grp": group, "dev": dev},
            device_id_type=MESH,
        )

    def dense_partial():
        for j in range(wide):
            part[pl.ds(j * hid, hid), :] = lax.dot_general(
                acts_ref[...],
                cot_ref[:, j * 128 : (j + 1) * 128],
                (((0,), (0,)), ((), ())),
                preferred_element_type=jnp.float32,
            )
        bpart[0] = jnp.zeros(bpart.shape[1:], jnp.float32)
        for j in range(wide):
            bpart[0, j : j + 1, :] = jnp.sum(
                cot_ref[:, j * 128 : (j + 1) * 128].astype(jnp.float32), axis=0, keepdims=True
            )

    near = me + 1 - 2 * core
    across = me + 2 - 4 * xbit
    stages = (
        (near, grp, core, half0),
        (across, grp, xbit, half1),
        (me, other, grp, half2),
    )
    bases = [0]
    for s in range(3):
        size = total >> (s + 1)
        bases.append(bases[s] + stages[s][2] * size)

    def halving(s):
        dev, group, bit, landing = stages[s]
        size = total >> (s + 1)
        away = pl.multiple_of(bases[s] + (1 - bit) * size, 8)
        return (
            remote(
                part.at[pl.ds(away, size)], landing, dsend.at[s], drecv.at[s], dev, group
            ),
            remote(bpart.at[s], bhalf.at[s], bsend.at[s], brecv.at[s], dev, group),
        )

    def halving_start(s):
        for copy in halving(s):
            copy.start()

    def halving_finish(s):
        for copy in halving(s):
            copy.wait()
        size = total >> (s + 1)
        keep = pl.multiple_of(bases[s + 1], 8)
        part[pl.ds(keep, size), :] = part[pl.ds(keep, size), :] + stages[s][3][...]
        bpart[s + 1] = bpart[s] + bhalf[s]

    piece = (total >> 3) // zs

    def z_copy(k):
        peer = lax.rem(z + k, zs)
        dev = peer * 4 + lax.rem(me, 4)
        away = pl.multiple_of(bases[3] + peer * piece, 8)
        return (
            remote(
                part.at[pl.ds(away, piece)], zbuf.at[z], zsend.at[peer], zrecv.at[z], dev, grp
            ),
            remote(bpart.at[3], bz.at[z], bsend.at[3 + peer], brecv.at[3 + z], dev, grp),
        )

    def z_wait(k):
        peer = lax.rem(z + k, zs)
        dev = peer * 4 + lax.rem(me, 4)
        here = pl.multiple_of(bases[3] + z * piece, 8)
        return (
            remote(
                part.at[pl.ds(here, piece)], zbuf.at[peer], zsend.at[peer], zrecv.at[peer], dev, grp
            ),
            remote(bpart.at[3], bz.at[peer], bsend.at[3 + peer], brecv.at[3 + peer], dev, grp),
        )

    mine = pl.multiple_of(bases[3] + z * piece, 8)

    def z_start():
        @pl.loop(1, zs)
        def _(k):
            for copy in z_copy(k):
                copy.start()

    def z_finish():
        zbuf[z] = part[pl.ds(mine, piece), :]
        bz[z] = bpart[3]

        @pl.loop(1, zs)
        def _(k):
            for copy in z_wait(k):
                copy.wait_recv()

        @pl.loop(1, zs)
        def _(k):
            for copy in z_copy(k):
                copy.wait_send()

        whole[pl.ds(mine, piece), :] = lax.fori_loop(
            1, zs, lambda i, run: run + zbuf[i], zbuf[0]
        )
        bsum = lax.fori_loop(1, zs, lambda i, run: run + bz[i], bz[0])
        for j in range(wide):
            bias_ref[:, j * 128 : (j + 1) * 128] = bsum[j : j + 1, :]

    def zg_copy(k, back):
        peer = lax.rem(z + k, zs)
        dev = peer * 4 + lax.rem(me, 4)
        off = mine if not back else pl.multiple_of(bases[3] + peer * piece, 8)
        block = whole.at[pl.ds(off, piece)]
        return remote(block, block, gsend.at[peer], grecv.at[peer if back else z], dev, grp)

    def zg_start():
        @pl.loop(1, zs)
        def _(k):
            zg_copy(k, False).start()

    def zg_finish():
        @pl.loop(1, zs)
        def _(k):
            zg_copy(k, True).wait_recv()

        @pl.loop(1, zs)
        def _(k):
            zg_copy(k, False).wait_send()

    def doubling(s, back):
        dev, group, bit, _ = stages[s]
        size = total >> (s + 1)
        off = bases[s] + (1 - bit) * size if back else bases[s + 1]
        block = whole.at[pl.ds(pl.multiple_of(off, 8), size)]
        return remote(block, block, esend.at[s], erecv.at[s], dev, group)

    def doubling_start(s):
        doubling(s, False).start()

    def doubling_finish(s):
        doubling(s, True).wait_recv()
        doubling(s, False).wait_send()

    place = lax.rem(me, 4)
    places = (
        place,
        place + 1 - 2 * core,
        place + 2 - 4 * xbit,
        place + 3 - 4 * xbit - 2 * core,
    )

    barrier = pltpu.get_barrier_semaphore()

    def greet(dev, group):
        pl.semaphore_signal(
            barrier, inc=1, device_id={"grp": group, "dev": dev}, device_id_type=MESH
        )

    for m in range(1, 4):
        greet(z * 4 + places[m], grp)

    @pl.loop(1, zs)
    def _(k):
        greet(lax.rem(z + k, zs) * 4 + place, grp)

    greet(me, other)
    pl.semaphore_wait(barrier, 3 + zs)

    def each_far(act):
        @pl.loop(1, zs)
        def _(i):
            for peer in (z + zs - i, z - zs + i):
                pl.when((peer >= 0) & (peer < zs))(functools.partial(act, peer))

    def each_near(act):
        @pl.loop(1, zs)
        def _(i):
            for peer in (z + i, z - i):
                pl.when((peer >= 0) & (peer < zs))(functools.partial(act, peer))

    def column_copy(m, peer):
        return remote(
            send.at[peer * 4 + places[m]],
            inter.at[m - 1, peer],
            psend.at[m - 1, peer],
            precv.at[m - 1, peer],
            z * 4 + places[m],
            grp,
        )

    def level_copy(m, back=False):
        who = z * 4 + places[m]
        return remote(
            send.at[who],
            recv.at[0, who if back else me],
            psend.at[m - 1, z],
            precv.at[m - 1, z],
            who,
            grp,
        )

    def line_copy(m, peer):
        origin = send.at[peer * 4 + place] if m == 0 else inter.at[m - 1, peer]
        return remote(
            origin,
            recv.at[0, z * 4 + places[m]],
            csend.at[m, peer],
            crecv.at[m, z],
            peer * 4 + place,
            grp,
        )

    def line_wait(m, peer):
        landing = recv.at[0, peer * 4 + places[m]]
        remote(
            landing, landing, csend.at[m, peer], crecv.at[m, peer], peer * 4 + place, grp
        ).wait_recv()

    def forward(src):
        return remote(
            recv.at[0, src], recv.at[1, src], fsend.at[src], frecv.at[src], me, other
        )

    def build(dst):
        digits = []
        for s in range(owned):
            t = slot_ref[dst * owned + s]
            send[dst, pl.ds(s * samples, samples), :] = x_ref[t]
            picked = ids_ref[t]
            digits += [picked >> DIGIT_BITS, picked & (DIGIT - 1)]
        send[dst, pl.ds(owned * samples, owned * id_rows), :] = jnp.concatenate(
            digits, axis=0
        ).astype(jnp.float32).astype(jnp.bfloat16)

    pl.loop(0, devs)(build)
    recv[0, me] = send[me]

    def column_start(m):
        each_far(lambda peer: column_copy(m, peer).start())
        level_copy(m).start()

    def column_pass(m):
        def act(peer):
            column_copy(m, peer).wait_recv()
            line_copy(m, peer).start()

        each_far(act)
        level_copy(m, True).wait_recv()
        forward(z * 4 + places[m]).start()

    each_far(lambda peer: line_copy(0, peer).start())
    column_start(2)
    column_start(1)
    forward(me).start()

    def accumulate(side, first, second):
        digits = jnp.concatenate(
            [
                recv[side, c, pl.ds(owned * samples, owned * id_rows), :].astype(jnp.float32)
                for c in (first, second)
            ],
            axis=1,
        )
        for s in range(owned):
            top = digits[s * id_rows : s * id_rows + pool]
            low = digits[s * id_rows + pool : s * id_rows + 2 * pool]
            rows = top * DIGIT + low
            values = jnp.concatenate(
                [recv[side, c, pl.ds(s * samples, samples), :] for c in (first, second)],
                axis=0,
            )
            for block in range(ROWS // ROW_BLOCK):
                local = rows - block * ROW_BLOCK
                local = jnp.where((local >= 0) & (local < ROW_BLOCK), local, -1.0).astype(
                    jnp.bfloat16
                )
                axis = lax.broadcasted_iota(
                    jnp.int32, (ROW_BLOCK, 2 * samples), 0
                ).astype(jnp.float32).astype(jnp.bfloat16)
                one, zero = jnp.bfloat16(1), jnp.bfloat16(0)
                counts = jnp.where(local[0:1] == axis, one, zero)
                for p in range(1, pool):
                    counts = counts + jnp.where(local[p : p + 1] == axis, one, zero)
                span = pl.ds(block * ROW_BLOCK, ROW_BLOCK)
                table_ref[s, span, :] = table_ref[s, span, :] + jnp.dot(
                    counts, values, preferred_element_type=jnp.float32
                )

    def pair(side, half, peer):
        accumulate(side, peer * 4 + places[2 * half], peer * 4 + places[2 * half + 1])

    def line_pass(m):
        def act(peer):
            line_wait(m, peer)
            forward(peer * 4 + places[m]).start()

        each_near(act)

    def own_pairs(half):
        pair(0, half, z)
        each_near(functools.partial(pair, 0, half))

    def far_pair(half, peer):
        for m in (2 * half, 2 * half + 1):
            forward(peer * 4 + places[m]).wait_recv()
        pair(1, half, peer)

    dense_partial()
    halving_start(0)
    column_pass(1)
    table_ref[...] = jnp.zeros(table_ref.shape, jnp.float32)
    halving_finish(0)
    halving_start(1)
    column_start(3)
    column_pass(2)
    line_pass(0)
    halving_finish(1)
    halving_start(2)
    line_pass(1)
    halving_finish(2)
    z_start()
    column_pass(3)
    own_pairs(0)
    line_pass(2)
    z_finish()
    zg_start()
    far_pair(0, z)
    line_pass(3)
    zg_finish()
    doubling_start(2)
    own_pairs(1)
    each_near(functools.partial(far_pair, 0))
    doubling_finish(2)
    doubling_start(1)
    far_pair(1, z)
    each_near(functools.partial(far_pair, 1))
    doubling_finish(1)
    doubling_start(0)
    doubling_finish(0)
    for j in range(wide):
        weight_ref[:, j * 128 : (j + 1) * 128] = whole[pl.ds(j * hid, hid), :]

    def drain(peer):
        for m in range(4):
            line_copy(m, peer).wait_send()
            if m > 0:
                column_copy(m, peer).wait_send()

    each_near(drain)
    for m in range(1, 4):
        level_copy(m).wait_send()

    @pl.loop(0, devs)
    def _(src):
        forward(src).wait_send()


def solution(mesh):
    devs = mesh.shape["dev"]

    def per_device(pooled_grad, row_ids, scale_exps, table_owner, dense_acts, dense_cot):
        samples, tables, feat = pooled_grad.shape
        pool = row_ids.shape[1]
        owned = tables // devs
        hid, hid2 = dense_acts.shape[1], dense_cot.shape[1]
        zs = devs // 4
        factor = powers(scale_exps)[:, :, None]
        restored = jnp.transpose(
            jnp.clip(pooled_grad.astype(jnp.float32), -factor, factor).astype(jnp.bfloat16),
            (1, 0, 2),
        )
        by_table = jnp.transpose(row_ids, (2, 1, 0))
        order = jnp.arange(tables, dtype=jnp.int32)
        slots = jnp.sum(
            jnp.where(table_owner[None, :] == order[:, None], order[None, :], 0), axis=1
        ).astype(jnp.int32)
        rows = owned * samples + owned * 2 * pool
        total = hid * hid2 // 128
        dma = pltpu.SemaphoreType.DMA
        vmem = pl.BlockSpec(memory_space=pltpu.VMEM)
        table_grad, weight_grad, bias_grad = pl.pallas_call(
            functools.partial(kernel, devs, pool),
            out_shape=(
                jax.ShapeDtypeStruct((owned, ROWS, feat), jnp.float32),
                jax.ShapeDtypeStruct((hid, hid2), jnp.float32),
                jax.ShapeDtypeStruct((1, hid2), jnp.float32),
            ),
            in_specs=[pl.BlockSpec(memory_space=pltpu.SMEM)] + [vmem] * 4,
            out_specs=(vmem, vmem, vmem),
            scratch_shapes=[
                pltpu.VMEM((devs, rows, feat), jnp.bfloat16),
                pltpu.VMEM((2, devs, rows, feat), jnp.bfloat16),
                pltpu.VMEM((3, zs, rows, feat), jnp.bfloat16),
                pltpu.VMEM((total, 128), jnp.float32),
                pltpu.VMEM((total, 128), jnp.float32),
                pltpu.VMEM((total // 2, 128), jnp.float32),
                pltpu.VMEM((total // 4, 128), jnp.float32),
                pltpu.VMEM((total // 8, 128), jnp.float32),
                pltpu.VMEM((zs, total // 8 // zs, 128), jnp.float32),
                pltpu.VMEM((4, 8, 128), jnp.float32),
                pltpu.VMEM((3, 8, 128), jnp.float32),
                pltpu.VMEM((zs, 8, 128), jnp.float32),
                dma((3, zs)),
                dma((3, zs)),
                dma((4, zs)),
                dma((4, zs)),
                dma((devs,)),
                dma((devs,)),
                dma((3,)),
                dma((3,)),
                dma((3,)),
                dma((3,)),
                dma((zs,)),
                dma((zs,)),
                dma((3 + zs,)),
                dma((3 + zs,)),
                dma((zs,)),
                dma((zs,)),
            ],
            compiler_params=pltpu.CompilerParams(collective_id=0, has_side_effects=True),
        )(slots, restored, by_table, dense_acts, dense_cot)
        return table_grad, weight_grad, bias_grad.reshape(hid2)

    return jax.shard_map(
        per_device,
        mesh=mesh,
        in_specs=(
            P(("grp", "dev"), None, None),
            P(("grp", "dev"), None, None),
            P(("grp", "dev"), None),
            P(),
            P(("grp", "dev"), None),
            P(("grp", "dev"), None),
        ),
        out_specs=(P("dev", None, None), P(), P()),
        check_vma=False,
    )
```
